32 devices in a mesh: seq: 4 (over z), nbr: 4 (over y, x), batch: 2 (over core).
Axes of the slice: x: 2, y: 2, z: 4, core: 2. Of those that a mesh axis runs over, the one named last changes fastest.
Arguments:
- hidden: bfloat16 [1024, 4096], P(('batch', 'seq'), 'nbr'), parts along dimension 0, may hold values from -6 to 6
- d_out: bfloat16 [1024, 4096], P(('batch', 'seq'), 'nbr'), parts along dimension 0, may hold values from -6 to 6
- nbr_emb: bfloat16 [192, 128, 896], P(('batch', 'seq', 'nbr')), parts along dimension 0, may hold values from -6 to 6
- slot_span: int32 [192], P(('batch', 'seq')), parts along dimension 0, may hold values from -1 to 1, as said below
- dec_gain: bfloat16 [4096], P('nbr'), may hold values from 0.5 to 1.5
- enc_gain: bfloat16 [896], replicated, may hold values from 0.5 to 1.5
- w_cond: bfloat16 [4096, 896], P('nbr'), may hold values from -0.75 to 0.75
- w_enc: bfloat16 [896, 896], replicated, may hold values from -0.1875 to 0.1875
- w_q: bfloat16 [4096, 2048], P('seq', 'nbr'), may hold values from -0.09375 to 0.09375
- w_k: bfloat16 [896, 2048], P('seq', 'nbr'), may hold values from -8 to 8
- w_v: bfloat16 [896, 2048], P('seq', 'nbr'), may hold values from -0.1875 to 0.1875
- w_o: bfloat16 [2048, 4096], P('nbr', 'seq'), may hold values from -0.125 to 0.125
Outputs:
- out: bfloat16 [1024, 4096], P(('batch', 'seq'), 'nbr'), parts along dimension 0
- d_hidden: bfloat16 [1024, 4096], P(('batch', 'seq'), 'nbr'), parts along dimension 0
- d_enc: bfloat16 [192, 128, 896], P(('batch', 'seq', 'nbr')), parts along dimension 0
- d_wo: float32 [4096, 4096], P(('batch', 'nbr'), 'seq'), parts along dimension 0
- d_wk: float32 [1792, 2048], P(('batch', 'seq'), 'nbr'), parts along dimension 0
- d_wv: float32 [1792, 2048], P(('batch', 'seq'), 'nbr'), parts along dimension 0
The draws below stay inside these ranges and needn't reach their ends.
There are 2 independent parts, one for each index of `batch`. The reference program is written for one: setup_inputs(seed, part) draws one part's arguments, and reference() takes and returns one part's arrays. A program takes and returns all parts, laid end to end along the dimension named above; an argument that names none is the same for every part. Nothing has to cross between parts.
Inputs may be any that keep to these rules, and one draw needn't show every extreme that they name: `slot_span`: A slot on seq index s serves a span of seq index s, counted from 0 within its 2 spans; -1 marks an empty slot. Every span is served by 1 to 8 slots, and one span of each seq index by exactly 8. Within each seq index one nbr index has all 6 slots live.
All inputs are finite; a program needn't handle non-finite values.
Results may differ from the reference program's by a relative error of at most 0.018.
The reference program's roundings to bfloat16 on the way count: a program that leaves them out, or rounds other values in their place, can miss the bound.
Values may be sent and summed in bfloat16 or wider, within the bound.
A program may use at most 128 MiB of HBM per device.

```python
import jax
import jax.numpy as jnp
from jax import lax

D = 4096
EW = 896
H = 16
HD = 128
CLEN = 64
NLEN = 128
KMAX = 8
NEIGHBOUR_SLOTS = 6
TOK_DEV = 128
TOKENS = 512
SPANS_PER_INDEX = 2
SPANS = 8
GSLOT = 24
SLOTS = 96
HW = 2048
N_SEQ = 4
N_NBR = 4


def draw_group_index(group_random_key):
    slot_count = NEIGHBOUR_SLOTS * N_NBR
    batch_random_key, occupy_random_key, order_random_key, first_random_key = jax.random.split(group_random_key, 4)
    draw_batch = jax.random.randint(batch_random_key, (), 0, SPANS_PER_INDEX)
    span_index = jnp.arange(slot_count, dtype=jnp.int32)
    remaining_slots = span_index - SPANS_PER_INDEX - KMAX + 1
    other_device = (draw_batch + 1 + remaining_slots % (SPANS_PER_INDEX - 1)) % SPANS_PER_INDEX
    occupied_slots = (jax.random.randint(occupy_random_key, (slot_count,), 0, 4) == 0) & (remaining_slots < (KMAX - 1) * (SPANS_PER_INDEX - 1))
    group_label = jnp.where(span_index < SPANS_PER_INDEX, span_index, jnp.where(remaining_slots < 0, draw_batch, jnp.where(occupied_slots, other_device, -1)))
    group_label = group_label.astype(jnp.int32)
    shuffle = jax.random.permutation(order_random_key, slot_count).astype(jnp.int32)
    ranked = jnp.where(group_label >= 0, 0, slot_count) + shuffle
    order = jnp.argsort(ranked)
    ordered = group_label[order]
    first_slot = jax.random.randint(first_random_key, (), 0, N_NBR)
    device_index = (span_index // NEIGHBOUR_SLOTS + first_slot) % N_NBR
    target_device = (device_index * NEIGHBOUR_SLOTS + span_index % NEIGHBOUR_SLOTS).astype(jnp.int32)
    return jnp.zeros((slot_count,), jnp.int32).at[target_device].set(ordered)


def draw_slot_span(key, part):
    group_key_list = jax.random.split(jax.random.fold_in(key, 17), N_SEQ)
    return jax.vmap(draw_group_index)(group_key_list).reshape(N_SEQ * NEIGHBOUR_SLOTS * N_NBR)


def draw_w_k(key, part):
    k_base, k_heads = jax.random.split(jax.random.fold_in(key, 29))
    base = jnp.clip(jax.random.normal(k_base, (EW, HW), jnp.float32), -4.0, 4.0) * EW ** (-0.5)
    picked = jax.random.permutation(k_heads, H)
    column_head = jnp.arange(HW, dtype=jnp.int32) // HD
    strength = jnp.where(column_head == picked[0], 2.5, 1.0)
    return jnp.clip(base * strength[None, :].astype(jnp.float32), -8.0, 8.0).astype(jnp.bfloat16)


def steps_of(own_key, dims, cuts, least, high):
    def one(dim, parts):
        draws = jax.random.uniform(jax.random.fold_in(jax.random.fold_in(own_key, 6), dim), (parts,), jnp.float32, least / len(cuts), high / len(cuts))
        return jnp.repeat(jnp.exp(draws), dims[dim] // parts).reshape((-1,) + (1,) * (len(dims) - dim - 1))

    factor_of = one(*cuts[0])
    for cut in cuts[1:]:
        factor_of = factor_of * one(*cut)
    return factor_of


def bell_draw(rng, dims, scale, bound, shards=(), kind=jnp.bfloat16):
    result = jax.random.normal(rng, dims, jnp.float32) * scale
    if len(shards) > 0:
        result = steps_of(rng, dims, shards, -0.22, 0.18) * result
    return jnp.clip(result, min=-bound, max=bound).astype(kind)


def setup_inputs(seed: int = 0, part: int = 0) -> dict:
    key_list = jax.random.split(jax.random.key(seed), 13)
    part_splits = jax.random.split(jax.random.fold_in(key_list[12], part), 13)
    hidden = bell_draw(part_splits[0], (TOKENS, D), 1.0, 6.0, ((0, 4), (1, 4)))
    d_out = bell_draw(part_splits[1], (TOKENS, D), 1.0, 6.0, ((0, 4), (1, 4)))
    nbr_emb = bell_draw(part_splits[2], (SLOTS, NLEN, EW), 1.0, 6.0, ((0, 16),))
    slot_span = draw_slot_span(jax.random.fold_in(jax.random.fold_in(key_list[12], part), 71), part)
    dec_gain = jnp.clip(1.0 + 0.1 * jax.random.normal(key_list[4], (D,), jnp.float32), 0.5, 1.5).astype(jnp.bfloat16)
    enc_gain = jnp.clip(1.0 + 0.1 * jax.random.normal(key_list[5], (EW,), jnp.float32), 0.5, 1.5).astype(jnp.bfloat16)
    w_cond = bell_draw(key_list[6], (D, EW), (D // 64) ** -0.5, 0.75, ((0, 4),))
    w_enc = bell_draw(key_list[7], (EW, EW), EW ** -0.5, 0.1875)
    w_q = bell_draw(key_list[8], (D, HW), D ** -0.5, 0.09375, ((0, 4), (1, 4)))
    w_k = draw_w_k(jax.random.fold_in(key_list[12], 71), part)
    w_v = bell_draw(key_list[10], (EW, HW), EW ** -0.5, 0.1875, ((0, 4), (1, 4)))
    w_o = bell_draw(key_list[11], (HW, D), HW ** -0.5, 0.125, ((0, 4), (1, 4)))
    return dict(hidden=hidden, d_out=d_out, nbr_emb=nbr_emb, slot_span=slot_span, dec_gain=dec_gain, enc_gain=enc_gain, w_cond=w_cond, w_enc=w_enc, w_q=w_q, w_k=w_k, w_v=w_v, w_o=w_o)


def rms_scale(values):
    return lax.rsqrt(lax.optimization_barrier(jnp.mean(values * values, axis=-1, keepdims=True)) + 1e-06)

def group_attention(operands):
    query, keys, values, d_attn, owners = operands
    factor = HD ** (-0.5)
    token_span = jnp.arange(TOK_DEV, dtype=jnp.int32) // CLEN
    key_span = jnp.repeat(owners, NLEN)
    allowed = token_span[:, None] == key_span[None, :]
    qf = query.astype(jnp.float32)
    kf = keys.astype(jnp.float32)
    vf = values.astype(jnp.float32)
    df = d_attn.astype(jnp.float32)
    scores = jnp.einsum('thd,khd->htk', qf, kf) * factor
    scores = jnp.where(allowed[None], scores, -1e+30)
    peak = lax.optimization_barrier(jnp.max(scores, axis=-1, keepdims=True))
    weights = jnp.exp(scores - peak)
    probs = weights / lax.optimization_barrier(jnp.sum(weights, axis=-1, keepdims=True))
    probs_b = probs.astype(jnp.bfloat16)
    pf = probs_b.astype(jnp.float32)
    attended = jnp.einsum('htk,khd->thd', pf, vf).astype(jnp.bfloat16)
    d_probs = jnp.einsum('thd,khd->htk', df, vf)
    row_dot = lax.optimization_barrier(jnp.sum(probs * d_probs, axis=-1, keepdims=True))
    d_scores = (probs * (d_probs - row_dot) * factor).astype(jnp.bfloat16).astype(jnp.float32)
    d_query = jnp.einsum('htk,khd->thd', d_scores, kf).astype(jnp.bfloat16)
    d_key = jnp.einsum('htk,thd->khd', d_scores, qf).astype(jnp.bfloat16)
    d_value = jnp.einsum('htk,thd->khd', pf, df).astype(jnp.bfloat16)
    return (attended, d_query, d_key, d_value)

def reference(hidden, d_out, nbr_emb, slot_span, dec_gain, enc_gain, w_cond, w_enc, w_q, w_k, w_v, w_o):
    hf = hidden.astype(jnp.float32)
    pooled = lax.optimization_barrier(jnp.mean(hf.reshape(SPANS, CLEN, D), axis=1)).astype(jnp.bfloat16)
    before = jnp.concatenate([jnp.zeros((1, D), jnp.bfloat16), pooled[:SPANS - 1]], axis=0)
    cond = jnp.dot(before, w_cond, preferred_element_type=jnp.float32)
    group_index = jnp.arange(SLOTS, dtype=jnp.int32) // GSLOT
    live = slot_span >= 0
    served = (group_index * SPANS_PER_INDEX + jnp.maximum(slot_span, 0)).astype(jnp.int32)
    slot_cond = jnp.where(live[:, None], cond[served], jnp.float32(0.0))
    inputs = nbr_emb.astype(jnp.float32) + slot_cond[:, None, :]
    enc_normed = (inputs * rms_scale(inputs) * enc_gain.astype(jnp.float32)).astype(jnp.bfloat16)
    mixed = jnp.dot(enc_normed.reshape(-1, EW), w_enc, preferred_element_type=jnp.float32).reshape(inputs.shape)
    encoded = (inputs + jax.nn.silu(mixed)).astype(jnp.bfloat16)
    enc_rows = encoded.reshape(-1, EW)
    rstd = rms_scale(hf)
    normed = (hf * rstd * dec_gain.astype(jnp.float32)).astype(jnp.bfloat16)
    query = jnp.dot(normed, w_q, preferred_element_type=jnp.float32).astype(jnp.bfloat16)
    keys = jnp.dot(enc_rows, w_k, preferred_element_type=jnp.float32).astype(jnp.bfloat16)
    values = jnp.dot(enc_rows, w_v, preferred_element_type=jnp.float32).astype(jnp.bfloat16)
    d_attn = jnp.dot(d_out, w_o.T, preferred_element_type=jnp.float32).astype(jnp.bfloat16)
    attended, d_query, d_key, d_value = lax.map(group_attention, (query.reshape(N_SEQ, TOK_DEV, H, HD), keys.reshape(N_SEQ, GSLOT * NLEN, H, HD), values.reshape(N_SEQ, GSLOT * NLEN, H, HD), d_attn.reshape(N_SEQ, TOK_DEV, H, HD), slot_span.reshape(N_SEQ, GSLOT)))
    attended = attended.reshape(TOKENS, HW)
    d_query = d_query.reshape(TOKENS, HW)
    d_key = d_key.reshape(SLOTS * NLEN, HW)
    d_value = d_value.reshape(SLOTS * NLEN, HW)
    out = (hf + jnp.dot(attended, w_o, preferred_element_type=jnp.float32)).astype(jnp.bfloat16)
    d_wo = jnp.dot(attended.T, d_out, preferred_element_type=jnp.float32)
    d_wk = jnp.dot(enc_rows.T, d_key, preferred_element_type=jnp.float32)
    d_wv = jnp.dot(enc_rows.T, d_value, preferred_element_type=jnp.float32)
    block = HW // N_NBR
    total = jnp.zeros((SLOTS * NLEN, EW), jnp.float32)
    for span_index in range(N_NBR):
        lower = span_index * block
        upper = lower + block
        part = jnp.dot(d_key[:, lower:upper], w_k[:, lower:upper].T, preferred_element_type=jnp.float32)
        part = part + jnp.dot(d_value[:, lower:upper], w_v[:, lower:upper].T, preferred_element_type=jnp.float32)
        total = total + part.astype(jnp.bfloat16).astype(jnp.float32)
    d_enc = total.reshape(SLOTS, NLEN, EW).astype(jnp.bfloat16)
    d_normed = jnp.dot(d_query, w_q.T, preferred_element_type=jnp.float32)
    scaled_grad = dec_gain.astype(jnp.float32) * d_normed
    stat = lax.optimization_barrier(jnp.mean(hf * scaled_grad, axis=-1, keepdims=True))
    d_hidden = (d_out.astype(jnp.float32) + rstd * scaled_grad - hf * rstd ** 3 * stat).astype(jnp.bfloat16)
    return (out, d_hidden, d_enc, d_wo, d_wk, d_wv)
```

```python
import functools

import jax
import jax.numpy as jnp
from jax import lax
from jax.experimental import pallas as pl
from jax.experimental.pallas import tpu as pltpu
from jax.sharding import PartitionSpec as P

HD = 128
CLEN = 64
NLEN = 128
KMAX = 8
BF = jnp.bfloat16
F32 = jnp.float32
MESH = pl.DeviceIdType.MESH
ANY = pl.BlockSpec(memory_space=pl.ANY)


def shifted(shard, axis, by):
    length = lax.axis_size(axis)
    pairs = [(i, i + by) for i in range(length) if 0 <= i + by < length]
    return lax.ppermute(shard, axis, pairs)


def rms_scale(values):
    return lax.rsqrt(jnp.mean(values * values, axis=-1, keepdims=True) + 1e-06)


def remote(src, dst, send, recv, dev):
    return pltpu.make_async_remote_copy(
        src_ref=src, dst_ref=dst, send_sem=send, recv_sem=recv, device_id=dev, device_id_type=MESH
    )


def cols(ref, i, width):
    return ref.at[:, pl.ds(pl.multiple_of(i * width, 128), width)]


def gather_kernel(n_seq, *refs):
    ins, outs, vm = refs[:8], refs[8:16], refs[16:24]
    lsem, osem, zs, zr, ps, pr, ns, nr = refs[24:]
    s, n, b = lax.axis_index("seq"), lax.axis_index("nbr"), lax.axis_index("batch")
    x, y, core = {"nbr": n ^ 1}, {"nbr": n ^ 2}, {"batch": 1 - b}
    right, left = {"seq": s + 1}, {"seq": s - 1}
    has_right, has_left = s + 1 < n_seq, s > 0

    def view(a, i):
        if a in (0, 1, 2):
            return cols(outs[a], i, ins[a].shape[1])
        if a == 7:
            return cols(outs[a], i, ins[a].shape[1])
        return outs[a].at[i]

    def half(a, ref, h):
        if a in (5, 6):
            w = ins[a].shape[1] // 2
            return cols(ref, h, w)
        rows = ins[a].shape[0] // 2
        return ref.at[pl.ds(h * rows, rows)]

    loads = [pltpu.make_async_copy(ins[a], vm[a], lsem.at[a]) for a in range(8)]
    for c in loads:
        c.start()
    barrier = pltpu.get_barrier_semaphore()
    for dev in (x, y, core):
        pl.semaphore_signal(barrier, inc=1, device_id=dev, device_id_type=MESH)

    for k in range(1, n_seq):
        dev = {"seq": lax.rem(s + k, n_seq)}
        pl.semaphore_signal(barrier, inc=1, device_id=dev, device_id_type=MESH)
    pl.semaphore_wait(barrier, n_seq + 2)

    def ring(a, k, d, src):
        own = s - k + 1 if d == 0 else s + k - 1
        dst = half(a, view(a, own), b)
        return remote(dst if src is None else src, dst, zs.at[a - 4, k, d], zr.at[a - 4, k, d],
                      right if d == 0 else left)

    def guard(d, k):
        if d == 0:
            return has_right & (s - (k - 1) >= 0)
        return has_left & (s + (k - 1) < n_seq)

    stores = []
    for a in (4, 7, 0, 1, 2, 3, 5, 6):
        loads[a].wait()
        c = pltpu.make_async_copy(vm[a], view(a, n if a < 4 else s), osem.at[a])
        c.start()
        stores.append(c)
        if a < 4:
            remote(vm[a], view(a, n), ns.at[a, 0], nr.at[a, 0], x).start()
            remote(vm[a], view(a, n), ns.at[a, 1], nr.at[a, 1], y).start()
        else:
            for d in (0, 1):
                @pl.when(guard(d, 1))
                def _(a=a, d=d):
                    ring(a, 1, d, half(a, vm[a], b)).start()

    def diagonal(a):
        for d, (src, dev, h) in enumerate(((n ^ 1, y, 0), (n ^ 2, x, 1))):
            full = view(a, src)
            remote(full, full, ns.at[a, d], nr.at[a, d], dev).wait_recv()
            part = half(a, full, h)
            remote(part, part, ns.at[a, 2 + d], nr.at[a, 2 + d], dev).start()

    def share(a, k, d, h):
        j = s - k if d == 0 else s + k
        part = half(a, view(a, j), h)
        return remote(part, part, ps.at[a - 4, k, d], pr.at[a - 4, k, d], core)

    def relay(a, k, d):
        valid = (s - k >= 0) if d == 0 else (s + k < n_seq)

        @pl.when(valid)
        def _():
            j = s - k if d == 0 else s + k
            part = half(a, view(a, j), b)
            remote(part, part, zs.at[a - 4, k, d], zr.at[a - 4, k, d],
                   left if d == 0 else right).wait_recv()
            share(a, k, d, b).start()

        if k + 1 < n_seq:
            @pl.when(guard(d, k + 1))
            def _():
                ring(a, k + 1, d, None).start()

    for a in (0, 1, 2):
        diagonal(a)
    for k in range(1, n_seq):
        for a in (4, 7, 5, 6):
            for d in (0, 1):
                relay(a, k, d)
        if k == 1:
            diagonal(3)
    for k in range(1, n_seq):
        for a in (4, 7, 5, 6):
            for d in (0, 1):
                @pl.when((s - k >= 0) if d == 0 else (s + k < n_seq))
                def _(a=a, k=k, d=d):
                    share(a, k, d, 1 - b).wait_recv()
                    share(a, k, d, b).wait_send()

                @pl.when(guard(d, k))
                def _(a=a, k=k, d=d):
                    ring(a, k, d, None).wait_send()
    for a in range(4):
        full = view(a, n ^ 3)
        for d in (0, 1):
            part = half(a, full, d)
            c = remote(part, part, ns.at[a, 2 + d], nr.at[a, 2 + d], x)
            c.wait_recv()
            c.wait_send()
            whole = view(a, n)
            remote(whole, whole, ns.at[a, d], nr.at[a, d], x).wait_send()
    for c in stores:
        c.wait()


def gather_all(hidden, d_out, gain, enc, w_q, w_k, w_v, w_o):
    n_seq, n_nbr = lax.axis_size("seq"), lax.axis_size("nbr")
    args = (hidden, d_out, gain, enc, w_q, w_k, w_v, w_o)
    shapes = []
    for i, v in enumerate(args):
        if i < 3:
            shape = (v.shape[0], v.shape[1] * n_nbr)
        elif i == 3:
            shape = (n_nbr,) + v.shape
        elif i < 7:
            shape = (n_seq,) + v.shape
        else:
            shape = (v.shape[0], v.shape[1] * n_seq)
        shapes.append(jax.ShapeDtypeStruct(shape, v.dtype))
    dma = pltpu.SemaphoreType.DMA
    return pl.pallas_call(
        functools.partial(gather_kernel, n_seq),
        out_shape=shapes,
        in_specs=[ANY] * 8,
        out_specs=[ANY] * 8,
        scratch_shapes=[pltpu.VMEM(v.shape, v.dtype) for v in args]
        + [dma((8,)), dma((8,)), dma((4, n_seq, 2)), dma((4, n_seq, 2)),
           dma((4, n_seq, 2)), dma((4, n_seq, 2)), dma((4, 4)), dma((4, 4))],
        compiler_params=pltpu.CompilerParams(
            collective_id=0, has_side_effects=True, vmem_limit_bytes=24 * 2**20
        ),
        name="gather_all",
    )(*args)


def exchange_kernel(n_seq, n_nbr, *refs):
    ins, outs = refs[:7], refs[7:14]
    ns, nr, zs, zr = refs[14:]
    s, n = lax.axis_index("seq"), lax.axis_index("nbr")
    barrier = pltpu.get_barrier_semaphore()
    for d in range(1, n_nbr):
        pl.semaphore_signal(barrier, inc=1, device_id={"nbr": lax.rem(n + d, n_nbr)}, device_id_type=MESH)
    for k in range(1, n_seq):
        pl.semaphore_signal(barrier, inc=1, device_id={"seq": lax.rem(s + k, n_seq)}, device_id_type=MESH)
    pl.semaphore_wait(barrier, n_nbr + n_seq - 2)
    copies = []
    for d in range(1, n_nbr):
        peer = lax.rem(n + d, n_nbr)
        for a in (2, 0, 1):
            if a == 2:
                src = ins[a].at[peer]
            else:
                src = cols(ins[a], peer, ins[a].shape[1] // n_nbr)
            copies.append(remote(src, outs[a].at[d - 1], ns.at[a, d], nr.at[a, d], {"nbr": peer}))
    for k in range(1, n_seq):
        peer = lax.rem(s + k, n_seq)
        for a in (3, 4, 5, 6):
            if a == 3:
                src = ins[a]
            elif a == 4:
                src = cols(ins[a], peer, ins[a].shape[1] // n_seq)
            else:
                src = ins[a].at[peer]
            copies.append(remote(src, outs[a].at[k - 1], zs.at[a - 3, k], zr.at[a - 3, k], {"seq": peer}))
    for c in copies:
        c.start()
    for c in copies:
        c.wait()


def exchange_all(part_out, part_dn, part_enc, attended, dout_all, part_wk, part_wv):
    n_seq, n_nbr = lax.axis_size("seq"), lax.axis_size("nbr")
    args = (part_out, part_dn, part_enc, attended, dout_all, part_wk, part_wv)
    tokens, full = part_out.shape
    shapes = [
        (n_nbr - 1, tokens, full // n_nbr),
        (n_nbr - 1, tokens, full // n_nbr),
        (n_nbr - 1,) + part_enc.shape[1:],
        (n_seq - 1,) + attended.shape,
        (n_seq - 1, tokens, full // n_seq),
        (n_seq - 1,) + part_wk.shape[1:],
        (n_seq - 1,) + part_wv.shape[1:],
    ]
    dma = pltpu.SemaphoreType.DMA
    return pl.pallas_call(
        functools.partial(exchange_kernel, n_seq, n_nbr),
        out_shape=[jax.ShapeDtypeStruct(v, BF) for v in shapes],
        in_specs=[ANY] * 7,
        out_specs=[ANY] * 7,
        scratch_shapes=[dma((3, n_nbr)), dma((3, n_nbr)), dma((4, n_seq)), dma((4, n_seq))],
        compiler_params=pltpu.CompilerParams(
            collective_id=1, has_side_effects=True, vmem_limit_bytes=8 * 2**20
        ),
        name="exchange_all",
    )(*args)


def project_kernel(idx, enc, wk, wv, enc_o, k_o, v_o):
    e = enc[0]
    enc_o[...] = e
    k_o[...] = jnp.dot(e, wk[...], preferred_element_type=F32).astype(BF)
    v_o[...] = jnp.dot(e, wv[...], preferred_element_type=F32).astype(BF)


def project(idx, enc, wk, wv):
    count, (width, local) = idx.shape[0], wk.shape
    out = lambda w: pl.BlockSpec((NLEN, w), lambda i, idx: (i, 0))
    weight = pl.BlockSpec((width, local), lambda i, idx: (0, 0))
    return pl.pallas_call(
        project_kernel,
        out_shape=[jax.ShapeDtypeStruct((count * NLEN, w), BF) for w in (width, local, local)],
        grid_spec=pltpu.PrefetchScalarGridSpec(
            num_scalar_prefetch=1,
            grid=(count,),
            in_specs=[pl.BlockSpec((1, NLEN, width), lambda i, idx: (idx[i], 0, 0)), weight, weight],
            out_specs=[out(width), out(local), out(local)],
        ),
        name="project",
    )(idx, enc, wk, wv)


NT = (((1,), (1,)), ((), ()))
TN = (((0,), (0,)), ((), ()))


def attend_kernel(counts, q_ref, k_ref, v_ref, da_ref, at_o, dq_o, dk_o, dv_o):
    q, k, v, da = q_ref[...], k_ref[...], v_ref[...], da_ref[...]
    factor = HD ** (-0.5)
    dot = functools.partial(lax.dot_general, preferred_element_type=F32)
    scores = dot(q, k, NT) * factor
    place = lax.broadcasted_iota(jnp.int32, scores.shape, 1)
    scores = jnp.where(place < counts[pl.program_id(0)] * NLEN, scores, -1e30)
    weights = jnp.exp(scores - jnp.max(scores, axis=-1, keepdims=True))
    probs = weights / jnp.sum(weights, axis=-1, keepdims=True)
    probs_b = probs.astype(BF)
    at_o[...] = jnp.dot(probs_b, v, preferred_element_type=F32).astype(BF)
    d_probs = dot(da, v, NT)
    row_dot = jnp.sum(probs * d_probs, axis=-1, keepdims=True)
    d_scores = (probs * (d_probs - row_dot) * factor).astype(BF)
    dq_o[...] = jnp.dot(d_scores, k, preferred_element_type=F32).astype(BF)
    dk_o[...] = dot(d_scores, q, TN).astype(BF)
    dv_o[...] = dot(probs_b, da, TN).astype(BF)


def attend(counts, query, keys, values, d_attn):
    tokens, local = query.shape
    spans = tokens // CLEN
    tok = pl.BlockSpec((CLEN, HD), lambda c, h, n: (c, h))
    key = pl.BlockSpec((KMAX * NLEN, HD), lambda c, h, n: (c, h))
    like = lambda v: jax.ShapeDtypeStruct(v.shape, BF)
    return pl.pallas_call(
        attend_kernel,
        out_shape=[like(query), like(query), like(keys), like(keys)],
        grid_spec=pltpu.PrefetchScalarGridSpec(
            num_scalar_prefetch=1,
            grid=(spans, local // HD),
            in_specs=[tok, key, key, tok],
            out_specs=[tok, tok, key, key],
        ),
        name="attend",
    )(counts, query, keys, values, d_attn)


def back_kernel(inv, dk, dv, wk, wv, o):
    live = inv[pl.program_id(0)] >= 0
    dot = functools.partial(lax.dot_general, preferred_element_type=F32)

    @pl.when(live)
    def _():
        o[0] = (dot(dk[...], wk[...], NT) + dot(dv[...], wv[...], NT)).astype(BF)

    @pl.when(jnp.logical_not(live))
    def _():
        o[0] = jnp.zeros(o.shape[1:], BF)


def back(inv, dk, dv, wk, wv):
    count, (width, local) = inv.shape[0], wk.shape
    row = pl.BlockSpec((NLEN, local), lambda i, inv: (jnp.maximum(inv[i], 0), 0))
    weight = pl.BlockSpec((width, local), lambda i, inv: (0, 0))
    return pl.pallas_call(
        back_kernel,
        out_shape=jax.ShapeDtypeStruct((count, NLEN, width), BF),
        grid_spec=pltpu.PrefetchScalarGridSpec(
            num_scalar_prefetch=1,
            grid=(count,),
            in_specs=[row, row, weight, weight],
            out_specs=pl.BlockSpec((1, NLEN, width), lambda i, inv: (i, 0, 0)),
        ),
        name="back",
    )(inv, dk, dv, wk, wv)


def body(hidden, d_out, nbr_emb, slot_span, dec_gain, enc_gain, w_cond, w_enc, w_q, w_k, w_v, w_o):
    s, n = lax.axis_index("seq"), lax.axis_index("nbr")
    tokens, feat = hidden.shape
    spans = tokens // CLEN
    pooled = jnp.mean(hidden.astype(F32).reshape(spans, CLEN, feat), axis=1).astype(BF)
    carried = shifted(pooled[spans - 1 :], "seq", 1)
    before = jnp.concatenate([carried, pooled[: spans - 1]], axis=0)
    condition = lax.psum(jnp.dot(before, w_cond, preferred_element_type=F32), "nbr")
    slots = nbr_emb.shape[0]
    own_span = lax.dynamic_slice_in_dim(slot_span, n * slots, slots)
    lookup = (own_span[:, None] == jnp.arange(spans, dtype=jnp.int32)[None, :]).astype(F32)
    slot_cond = jnp.dot(lookup, condition, precision=lax.Precision.HIGHEST)
    inputs = nbr_emb.astype(F32) + slot_cond[:, None, :]
    width = inputs.shape[2]
    enc_normed = (inputs * rms_scale(inputs) * enc_gain.astype(F32)).astype(BF)
    mixed = jnp.dot(enc_normed.reshape(-1, width), w_enc, preferred_element_type=F32).reshape(
        inputs.shape
    )
    encoded = (inputs + jax.nn.silu(mixed)).astype(BF)
    gain_rows = jnp.broadcast_to(dec_gain[None], (32, feat))
    hid_all, dout_all, gain_all, enc_all, wq_all, wk_all, wv_all, wo_all = gather_all(
        hidden, d_out, gain_rows, encoded, w_q, w_k, w_v, w_o
    )
    local = w_q.shape[1]
    wq_all = wq_all.reshape(-1, local)
    wk_all = wk_all.reshape(-1, local)
    wv_all = wv_all.reshape(-1, local)
    enc_all = enc_all.reshape(-1, NLEN, width)
    total = slot_span.shape[0]

    member = slot_span[None, :] == jnp.arange(spans, dtype=jnp.int32)[:, None]
    ids = jnp.arange(total, dtype=jnp.int32)
    earlier = ids[None, :] < ids[:, None]
    rank = jnp.sum((member[:, None, :] & earlier[None]).astype(jnp.int32), axis=-1)
    counts = jnp.sum(member.astype(jnp.int32), axis=-1)
    chosen = member[:, None, :] & (
        rank[:, None, :] == jnp.arange(KMAX, dtype=jnp.int32)[None, :, None]
    )
    idx = jnp.sum(jnp.where(chosen, ids[None, None, :], 0), axis=-1).reshape(-1)
    base = jnp.arange(spans, dtype=jnp.int32)[:, None] * KMAX
    inv = jnp.sum(jnp.where(member, base + rank + 1, 0), axis=0) - 1

    enc_rows, keys, values = project(idx, enc_all, wk_all, wv_all)
    hf = hid_all.astype(F32)
    rstd = rms_scale(hf)
    normed = (hf * rstd * gain_all[:1].astype(F32)).astype(BF)
    query = jnp.dot(normed, wq_all, preferred_element_type=F32).astype(BF)
    d_attn = lax.dot_general(dout_all, wo_all, NT, preferred_element_type=F32).astype(BF)
    attended, d_query, d_key, d_value = attend(counts, query, keys, values, d_attn)
    part_out = jnp.dot(attended, wo_all, preferred_element_type=F32).astype(BF)
    part_dn = lax.dot_general(d_query, wq_all, NT, preferred_element_type=F32).astype(BF)
    part_enc = back(inv, d_key, d_value, wk_all, wv_all).reshape((-1,) + nbr_emb.shape)
    rows = w_k.shape[0]
    part_wk = lax.dot_general(enc_rows, d_key, TN, preferred_element_type=F32).astype(BF)
    part_wv = lax.dot_general(enc_rows, d_value, TN, preferred_element_type=F32).astype(BF)
    part_wk = part_wk.reshape(-1, rows, local)
    part_wv = part_wv.reshape(-1, rows, local)
    out_r, dn_r, enc_r, att_r, col_r, wk_r, wv_r = exchange_all(
        part_out, part_dn, part_enc, attended, dout_all, part_wk, part_wv
    )

    def total_of(own, received):
        acc = own.astype(F32)
        for i in range(received.shape[0]):
            acc = acc + received[i].astype(F32)
        return acc

    def own_cols(v, i, w):
        return lax.dynamic_slice_in_dim(v, i * w, w, axis=1)

    def own_row(v, i):
        return lax.dynamic_index_in_dim(v, i, 0, keepdims=False)

    own_states = hidden.astype(F32)
    out = (own_states + total_of(own_cols(part_out, n, feat), out_r)).astype(BF)
    d_enc = total_of(own_row(part_enc, n), enc_r).astype(BF)
    d_wk = total_of(own_row(part_wk, s), wk_r)
    d_wv = total_of(own_row(part_wv, s), wv_r)
    piece = w_o.shape[1]
    d_wo = lax.dot_general(
        jnp.concatenate([attended[None], att_r]).reshape(-1, local),
        jnp.concatenate([own_cols(dout_all, s, piece)[None], col_r]).reshape(-1, piece),
        TN, preferred_element_type=F32)
    scaled_grad = dec_gain.astype(F32) * total_of(own_cols(part_dn, n, feat), dn_r)
    stat = lax.psum(jnp.sum(own_states * scaled_grad, axis=-1, keepdims=True) / hf.shape[1], "nbr")
    d_hidden = d_out.astype(F32) + rstd * scaled_grad - own_states * rstd**3 * stat
    return (out, d_hidden.astype(BF), d_enc, d_wo, d_wk, d_wv)


def solution(mesh):
    placed = (
        P(("batch", "seq"), "nbr"),
        P(("batch", "seq"), "nbr"),
        P(("batch", "seq", "nbr"), None, None),
        P(("batch", "seq")),
        P("nbr"),
        P(),
        P("nbr", None),
        P(),
        P("seq", "nbr"),
        P("seq", "nbr"),
        P("seq", "nbr"),
        P("nbr", "seq"),
    )
    return jax.shard_map(
        body,
        mesh=mesh,
        in_specs=placed,
        out_specs=(
            P(("batch", "seq"), "nbr"),
            P(("batch", "seq"), "nbr"),
            P(("batch", "seq", "nbr"), None, None),
            P(("batch", "nbr"), "seq"),
            P(("batch", "seq"), "nbr"),
            P(("batch", "seq"), "nbr"),
        ),
        check_vma=False,
    )
```

```python
import functools

import jax
import jax.numpy as jnp
from jax import lax
from jax.experimental import pallas as pl
from jax.experimental.pallas import tpu as pltpu
from jax.sharding import PartitionSpec as P

HD = 128
CLEN = 64
NLEN = 128
KMAX = 8
BF = jnp.bfloat16
F32 = jnp.float32
MESH = pl.DeviceIdType.MESH
ANY = pl.BlockSpec(memory_space=pl.ANY)


def shifted(shard, axis, by):
    length = lax.axis_size(axis)
    pairs = [(i, i + by) for i in range(length) if 0 <= i + by < length]
    return lax.ppermute(shard, axis, pairs)


def rms_scale(values):
    return lax.rsqrt(jnp.mean(values * values, axis=-1, keepdims=True) + 1e-06)


def remote(src, dst, send, recv, dev):
    return pltpu.make_async_remote_copy(
        src_ref=src, dst_ref=dst, send_sem=send, recv_sem=recv, device_id=dev, device_id_type=MESH
    )


def cols(ref, i, width):
    return ref.at[:, pl.ds(pl.multiple_of(i * width, 128), width)]


def gather_kernel(n_seq, *refs):
    ins, outs, vm = refs[:8], refs[8:16], refs[16:24]
    lsem, osem, zs, zr, ps, pr, ns, nr = refs[24:]
    s, n, b = lax.axis_index("seq"), lax.axis_index("nbr"), lax.axis_index("batch")
    x, y, core = {"nbr": n ^ 1}, {"nbr": n ^ 2}, {"batch": 1 - b}
    right, left = {"seq": s + 1}, {"seq": s - 1}
    has_right, has_left = s + 1 < n_seq, s > 0

    def view(a, i):
        if a in (0, 1, 2):
            return cols(outs[a], i, ins[a].shape[1])
        if a == 7:
            return cols(outs[a], i, ins[a].shape[1])
        return outs[a].at[i]

    def half(a, ref, h):
        if a in (5, 6):
            w = ins[a].shape[1] // 2
            return cols(ref, h, w)
        rows = ins[a].shape[0] // 2
        return ref.at[pl.ds(h * rows, rows)]

    loads = [pltpu.make_async_copy(ins[a], vm[a], lsem.at[a]) for a in range(8)]
    for c in loads:
        c.start()
    barrier = pltpu.get_barrier_semaphore()
    for dev in (x, y, core):
        pl.semaphore_signal(barrier, inc=1, device_id=dev, device_id_type=MESH)

    for k in range(1, n_seq):
        dev = {"seq": lax.rem(s + k, n_seq)}
        pl.semaphore_signal(barrier, inc=1, device_id=dev, device_id_type=MESH)
    pl.semaphore_wait(barrier, n_seq + 2)

    def ring(a, k, d, src):
        own = s - k + 1 if d == 0 else s + k - 1
        dst = half(a, view(a, own), b)
        return remote(dst if src is None else src, dst, zs.at[a - 4, k, d], zr.at[a - 4, k, d],
                      right if d == 0 else left)

    def guard(d, k):
        if d == 0:
            return has_right & (s - (k - 1) >= 0)
        return has_left & (s + (k - 1) < n_seq)

    stores = []
    for a in (4, 7, 0, 1, 2, 3, 5, 6):
        loads[a].wait()
        c = pltpu.make_async_copy(vm[a], view(a, n if a < 4 else s), osem.at[a])
        c.start()
        stores.append(c)
        if a < 4:
            remote(vm[a], view(a, n), ns.at[a, 0], nr.at[a, 0], x).start()
            remote(vm[a], view(a, n), ns.at[a, 1], nr.at[a, 1], y).start()
        else:
            for d in (0, 1):
                @pl.when(guard(d, 1))
                def _(a=a, d=d):
                    ring(a, 1, d, half(a, vm[a], b)).start()

    def diagonal(a):
        for d, (src, dev, h) in enumerate(((n ^ 1, y, 0), (n ^ 2, x, 1))):
            full = view(a, src)
            remote(full, full, ns.at[a, d], nr.at[a, d], dev).wait_recv()
            part = half(a, full, h)
            remote(part, part, ns.at[a, 2 + d], nr.at[a, 2 + d], dev).start()

    def share(a, k, d, h):
        j = s - k if d == 0 else s + k
        part = half(a, view(a, j), h)
        return remote(part, part, ps.at[a - 4, k, d], pr.at[a - 4, k, d], core)

    def relay(a, k, d):
        valid = (s - k >= 0) if d == 0 else (s + k < n_seq)

        @pl.when(valid)
        def _():
            j = s - k if d == 0 else s + k
            part = half(a, view(a, j), b)
            remote(part, part, zs.at[a - 4, k, d], zr.at[a - 4, k, d],
                   left if d == 0 else right).wait_recv()
            share(a, k, d, b).start()

        if k + 1 < n_seq:
            @pl.when(guard(d, k + 1))
            def _():
                ring(a, k + 1, d, None).start()

    for a in (0, 1, 2):
        diagonal(a)
    for k in range(1, n_seq):
        for a in (4, 7, 5, 6):
            for d in (0, 1):
                relay(a, k, d)
        if k == 1:
            diagonal(3)
    for k in range(1, n_seq):
        for a in (4, 7, 5, 6):
            for d in (0, 1):
                @pl.when((s - k >= 0) if d == 0 else (s + k < n_seq))
                def _(a=a, k=k, d=d):
                    share(a, k, d, 1 - b).wait_recv()
                    share(a, k, d, b).wait_send()

                @pl.when(guard(d, k))
                def _(a=a, k=k, d=d):
                    ring(a, k, d, None).wait_send()
    for a in range(4):
        full = view(a, n ^ 3)
        for d in (0, 1):
            part = half(a, full, d)
            c = remote(part, part, ns.at[a, 2 + d], nr.at[a, 2 + d], x)
            c.wait_recv()
            c.wait_send()
            whole = view(a, n)
            remote(whole, whole, ns.at[a, d], nr.at[a, d], x).wait_send()
    for c in stores:
        c.wait()


def gather_all(hidden, d_out, gain, enc, w_q, w_k, w_v, w_o):
    n_seq, n_nbr = lax.axis_size("seq"), lax.axis_size("nbr")
    args = (hidden, d_out, gain, enc, w_q, w_k, w_v, w_o)
    shapes = []
    for i, v in enumerate(args):
        if i < 3:
            shape = (v.shape[0], v.shape[1] * n_nbr)
        elif i == 3:
            shape = (n_nbr,) + v.shape
        elif i < 7:
            shape = (n_seq,) + v.shape
        else:
            shape = (v.shape[0], v.shape[1] * n_seq)
        shapes.append(jax.ShapeDtypeStruct(shape, v.dtype))
    dma = pltpu.SemaphoreType.DMA
    return pl.pallas_call(
        functools.partial(gather_kernel, n_seq),
        out_shape=shapes,
        in_specs=[ANY] * 8,
        out_specs=[ANY] * 8,
        scratch_shapes=[pltpu.VMEM(v.shape, v.dtype) for v in args]
        + [dma((8,)), dma((8,)), dma((4, n_seq, 2)), dma((4, n_seq, 2)),
           dma((4, n_seq, 2)), dma((4, n_seq, 2)), dma((4, 4)), dma((4, 4))],
        compiler_params=pltpu.CompilerParams(
            collective_id=0, has_side_effects=True, vmem_limit_bytes=24 * 2**20
        ),
        name="gather_all",
    )(*args)


def exchange_kernel(n_seq, n_nbr, *refs):
    ins, outs, transit = refs[:8], refs[8:16], refs[16]
    ns, nr, zs, zr, ts, tr, fs, fr = refs[17:]
    s, n = lax.axis_index("seq"), lax.axis_index("nbr")
    x, y = {"nbr": n ^ 1}, {"nbr": n ^ 2}
    barrier = pltpu.get_barrier_semaphore()
    for d in range(1, n_nbr):
        pl.semaphore_signal(barrier, inc=1, device_id={"nbr": n ^ d}, device_id_type=MESH)
    for k in range(1, n_seq):
        pl.semaphore_signal(barrier, inc=1, device_id={"seq": lax.rem(s + k, n_seq)}, device_id_type=MESH)
    pl.semaphore_wait(barrier, n_nbr + n_seq - 2)
    h = ins[2].shape[1] // 2
    parts = (pl.ds(0, h), pl.ds(h, h))
    hops = [
        remote(ins[2].at[n ^ 3, parts[i]], transit.at[i], ts.at[i], tr.at[i], dev)
        for i, dev in enumerate((x, y))
    ]
    for c in hops:
        c.start()
    copies = []
    for a in (2, 7, 0, 1):
        for d in (1, 2, 3):
            if a == 2 and d == 3:
                continue
            peer = n ^ d
            if a == 2:
                src = ins[a].at[peer]
            elif a == 7:
                src = ins[a]
            else:
                src = cols(ins[a], peer, ins[a].shape[1] // n_nbr)
            i = 3 if a == 7 else a
            copies.append(remote(src, outs[a].at[d - 1], ns.at[i, d], nr.at[i, d], {"nbr": peer}))
    for k in range(1, n_seq):
        peer = lax.rem(s + k, n_seq)
        for a in (3, 4, 5, 6):
            if a == 3:
                src = ins[a]
            elif a == 4:
                src = cols(ins[a], peer, ins[a].shape[1] // n_seq)
            else:
                src = ins[a].at[peer]
            copies.append(remote(src, outs[a].at[k - 1], zs.at[a - 3, k], zr.at[a - 3, k], {"seq": peer}))
    for c in copies:
        c.start()
    onward = []
    for i, dev in enumerate((y, x)):
        hops[i].wait_recv()
        c = remote(transit.at[i], outs[2].at[2, parts[i]], fs.at[i], fr.at[i], dev)
        c.start()
        onward.append(c)
    for c in copies + onward:
        c.wait()
    for c in hops:
        c.wait_send()


def exchange_all(part_out, part_dn, part_enc, attended, dout_all, part_wk, part_wv, part_stat):
    n_seq, n_nbr = lax.axis_size("seq"), lax.axis_size("nbr")
    args = (part_out, part_dn, part_enc, attended, dout_all, part_wk, part_wv, part_stat)
    tokens, full = part_out.shape
    slots = part_enc.shape[1:]
    shapes = [
        (n_nbr - 1, tokens, full // n_nbr),
        (n_nbr - 1, tokens, full // n_nbr),
        (n_nbr - 1,) + slots,
        (n_seq - 1,) + attended.shape,
        (n_seq - 1, tokens, full // n_seq),
        (n_seq - 1,) + part_wk.shape[1:],
        (n_seq - 1,) + part_wv.shape[1:],
        (n_nbr - 1,) + part_stat.shape,
        (2, slots[0] // 2) + slots[1:],
    ]
    types = [BF] * 7 + [F32, BF]
    dma = pltpu.SemaphoreType.DMA
    return pl.pallas_call(
        functools.partial(exchange_kernel, n_seq, n_nbr),
        out_shape=[jax.ShapeDtypeStruct(v, k) for v, k in zip(shapes, types)],
        in_specs=[ANY] * 8,
        out_specs=[ANY] * 9,
        scratch_shapes=[dma((4, n_nbr)), dma((4, n_nbr)), dma((4, n_seq)), dma((4, n_seq))]
        + [dma((2,))] * 4,
        compiler_params=pltpu.CompilerParams(
            collective_id=1, has_side_effects=True, vmem_limit_bytes=60 * 2**20
        ),
        name="exchange_all",
    )(*args)[:8]


GROUP = 4


def project_kernel(idx, *refs):
    wk, wv, enc_o, k_o, v_o = refs[GROUP:]
    e = jnp.concatenate([r[0] for r in refs[:GROUP]], axis=0)
    enc_o[...] = e
    k_o[...] = jnp.dot(e, wk[...], preferred_element_type=F32).astype(BF)
    v_o[...] = jnp.dot(e, wv[...], preferred_element_type=F32).astype(BF)


def project(idx, enc, wk, wv):
    count, (width, local) = idx.shape[0], wk.shape
    out = lambda w: pl.BlockSpec((GROUP * NLEN, w), lambda i, idx: (i, 0))
    weight = pl.BlockSpec((width, local), lambda i, idx: (0, 0))
    slot = lambda j: pl.BlockSpec((1, NLEN, width), lambda i, idx: (idx[i * GROUP + j], 0, 0))
    return pl.pallas_call(
        project_kernel,
        out_shape=[jax.ShapeDtypeStruct((count * NLEN, w), BF) for w in (width, local, local)],
        grid_spec=pltpu.PrefetchScalarGridSpec(
            num_scalar_prefetch=1,
            grid=(count // GROUP,),
            in_specs=[slot(j) for j in range(GROUP)] + [weight, weight],
            out_specs=[out(width), out(local), out(local)],
        ),
        name="project",
    )(idx, *([enc] * GROUP), wk, wv)


NT = (((1,), (1,)), ((), ()))
TN = (((0,), (0,)), ((), ()))


def attend_kernel(counts, q_ref, k_ref, v_ref, da_ref, at_o, dq_o, dk_o, dv_o):
    q, k, v, da = q_ref[...], k_ref[...], v_ref[...], da_ref[...]
    factor = HD ** (-0.5)
    dot = functools.partial(lax.dot_general, preferred_element_type=F32)
    scores = dot(q, k, NT) * factor
    place = lax.broadcasted_iota(jnp.int32, scores.shape, 1)
    scores = jnp.where(place < counts[pl.program_id(0)] * NLEN, scores, -1e30)
    weights = jnp.exp(scores - jnp.max(scores, axis=-1, keepdims=True))
    probs = weights / jnp.sum(weights, axis=-1, keepdims=True)
    probs_b = probs.astype(BF)
    at_o[...] = jnp.dot(probs_b, v, preferred_element_type=F32).astype(BF)
    d_probs = dot(da, v, NT)
    row_dot = jnp.sum(probs * d_probs, axis=-1, keepdims=True)
    d_scores = (probs * (d_probs - row_dot) * factor).astype(BF)
    dq_o[...] = jnp.dot(d_scores, k, preferred_element_type=F32).astype(BF)
    dk_o[...] = dot(d_scores, q, TN).astype(BF)
    dv_o[...] = dot(probs_b, da, TN).astype(BF)


def attend(counts, query, keys, values, d_attn):
    tokens, local = query.shape
    spans = tokens // CLEN
    tok = pl.BlockSpec((CLEN, HD), lambda c, h, n: (c, h))
    key = pl.BlockSpec((KMAX * NLEN, HD), lambda c, h, n: (c, h))
    like = lambda v: jax.ShapeDtypeStruct(v.shape, BF)
    return pl.pallas_call(
        attend_kernel,
        out_shape=[like(query), like(query), like(keys), like(keys)],
        grid_spec=pltpu.PrefetchScalarGridSpec(
            num_scalar_prefetch=1,
            grid=(spans, local // HD),
            in_specs=[tok, key, key, tok],
            out_specs=[tok, tok, key, key],
        ),
        name="attend",
    )(counts, query, keys, values, d_attn)


def back_kernel(inv, *refs):
    wk, wv, o = refs[2 * GROUP :]
    dot = functools.partial(lax.dot_general, preferred_element_type=F32)
    dk = jnp.concatenate([r[...] for r in refs[:GROUP]], axis=0)
    dv = jnp.concatenate([r[...] for r in refs[GROUP : 2 * GROUP]], axis=0)
    part = (dot(dk, wk[...], NT) + dot(dv, wv[...], NT)).astype(BF)
    for j in range(GROUP):
        live = inv[pl.program_id(0) * GROUP + j] >= 0
        rows = part[j * NLEN : (j + 1) * NLEN]
        o[j] = jnp.where(live, rows, jnp.zeros_like(rows))


def back(inv, dk, dv, wk, wv):
    count, (width, local) = inv.shape[0], wk.shape
    row = lambda j: pl.BlockSpec((NLEN, local), lambda i, inv: (jnp.maximum(inv[i * GROUP + j], 0), 0))
    weight = pl.BlockSpec((width, local), lambda i, inv: (0, 0))
    rows = [row(j) for j in range(GROUP)]
    return pl.pallas_call(
        back_kernel,
        out_shape=jax.ShapeDtypeStruct((count, NLEN, width), BF),
        grid_spec=pltpu.PrefetchScalarGridSpec(
            num_scalar_prefetch=1,
            grid=(count // GROUP,),
            in_specs=rows + rows + [weight, weight],
            out_specs=pl.BlockSpec((GROUP, NLEN, width), lambda i, inv: (i, 0, 0)),
        ),
        name="back",
    )(inv, *([dk] * GROUP), *([dv] * GROUP), wk, wv)


def body(hidden, d_out, nbr_emb, slot_span, dec_gain, enc_gain, w_cond, w_enc, w_q, w_k, w_v, w_o):
    s, n = lax.axis_index("seq"), lax.axis_index("nbr")
    tokens, feat = hidden.shape
    spans = tokens // CLEN
    pooled = jnp.mean(hidden.astype(F32).reshape(spans, CLEN, feat), axis=1).astype(BF)
    carried = shifted(pooled[spans - 1 :], "seq", 1)
    before = jnp.concatenate([carried, pooled[: spans - 1]], axis=0)
    condition = lax.psum(jnp.dot(before, w_cond, preferred_element_type=F32), "nbr")
    slots = nbr_emb.shape[0]
    own_span = lax.dynamic_slice_in_dim(slot_span, n * slots, slots)
    lookup = (own_span[:, None] == jnp.arange(spans, dtype=jnp.int32)[None, :]).astype(F32)
    slot_cond = jnp.dot(lookup, condition, precision=lax.Precision.HIGHEST)
    inputs = nbr_emb.astype(F32) + slot_cond[:, None, :]
    width = inputs.shape[2]
    enc_normed = (inputs * rms_scale(inputs) * enc_gain.astype(F32)).astype(BF)
    mixed = jnp.dot(enc_normed.reshape(-1, width), w_enc, preferred_element_type=F32).reshape(
        inputs.shape
    )
    encoded = (inputs + jax.nn.silu(mixed)).astype(BF)
    gain_rows = jnp.broadcast_to(dec_gain[None], (32, feat))
    hid_all, dout_all, gain_all, enc_all, wq_all, wk_all, wv_all, wo_all = gather_all(
        hidden, d_out, gain_rows, encoded, w_q, w_k, w_v, w_o
    )
    local = w_q.shape[1]
    wq_all = wq_all.reshape(-1, local)
    wk_all = wk_all.reshape(-1, local)
    wv_all = wv_all.reshape(-1, local)
    enc_all = enc_all.reshape(-1, NLEN, width)
    total = slot_span.shape[0]

    member = slot_span[None, :] == jnp.arange(spans, dtype=jnp.int32)[:, None]
    ids = jnp.arange(total, dtype=jnp.int32)
    earlier = ids[None, :] < ids[:, None]
    rank = jnp.sum((member[:, None, :] & earlier[None]).astype(jnp.int32), axis=-1)
    counts = jnp.sum(member.astype(jnp.int32), axis=-1)
    chosen = member[:, None, :] & (
        rank[:, None, :] == jnp.arange(KMAX, dtype=jnp.int32)[None, :, None]
    )
    idx = jnp.sum(jnp.where(chosen, ids[None, None, :], 0), axis=-1).reshape(-1)
    base = jnp.arange(spans, dtype=jnp.int32)[:, None] * KMAX
    inv = jnp.sum(jnp.where(member, base + rank + 1, 0), axis=0) - 1

    enc_rows, keys, values = project(idx, enc_all, wk_all, wv_all)
    hf = hid_all.astype(F32)
    rstd = rms_scale(hf)
    normed = (hf * rstd * gain_all[:1].astype(F32)).astype(BF)
    query = jnp.dot(normed, wq_all, preferred_element_type=F32).astype(BF)
    d_attn = lax.dot_general(dout_all, wo_all, NT, preferred_element_type=F32).astype(BF)
    attended, d_query, d_key, d_value = attend(counts, query, keys, values, d_attn)
    part_out = jnp.dot(attended, wo_all, preferred_element_type=F32).astype(BF)
    part_dn = lax.dot_general(d_query, wq_all, NT, preferred_element_type=F32).astype(BF)
    part_enc = back(inv, d_key, d_value, wk_all, wv_all).reshape((-1,) + nbr_emb.shape)
    rows = w_k.shape[0]
    part_wk = lax.dot_general(enc_rows, d_key, TN, preferred_element_type=F32).astype(BF)
    part_wv = lax.dot_general(enc_rows, d_value, TN, preferred_element_type=F32).astype(BF)
    part_wk = part_wk.reshape(-1, rows, local)
    part_wv = part_wv.reshape(-1, rows, local)
    part_stat = jnp.sum(
        hf * (gain_all[:1].astype(F32) * part_dn.astype(F32)), axis=-1, keepdims=True
    ) / hf.shape[1]
    part_stat = jnp.broadcast_to(part_stat, (tokens, HD))
    out_r, dn_r, enc_r, att_r, col_r, wk_r, wv_r, stat_r = exchange_all(
        part_out, part_dn, part_enc, attended, dout_all, part_wk, part_wv, part_stat
    )

    def total_of(own, received):
        acc = own.astype(F32)
        for i in range(received.shape[0]):
            acc = acc + received[i].astype(F32)
        return acc

    def own_cols(v, i, w):
        return lax.dynamic_slice_in_dim(v, i * w, w, axis=1)

    def own_row(v, i):
        return lax.dynamic_index_in_dim(v, i, 0, keepdims=False)

    own_states = hidden.astype(F32)
    out = (own_states + total_of(own_cols(part_out, n, feat), out_r)).astype(BF)
    d_enc = total_of(own_row(part_enc, n), enc_r).astype(BF)
    d_wk = total_of(own_row(part_wk, s), wk_r)
    d_wv = total_of(own_row(part_wv, s), wv_r)
    piece = w_o.shape[1]
    d_wo = lax.dot_general(
        jnp.concatenate([attended[None], att_r]).reshape(-1, local),
        jnp.concatenate([own_cols(dout_all, s, piece)[None], col_r]).reshape(-1, piece),
        TN, preferred_element_type=F32)
    scaled_grad = dec_gain.astype(F32) * total_of(own_cols(part_dn, n, feat), dn_r)
    stat = total_of(part_stat, stat_r)[:, :1]
    d_hidden = d_out.astype(F32) + rstd * scaled_grad - own_states * rstd**3 * stat
    return (out, d_hidden.astype(BF), d_enc, d_wo, d_wk, d_wv)


def solution(mesh):
    placed = (
        P(("batch", "seq"), "nbr"),
        P(("batch", "seq"), "nbr"),
        P(("batch", "seq", "nbr"), None, None),
        P(("batch", "seq")),
        P("nbr"),
        P(),
        P("nbr", None),
        P(),
        P("seq", "nbr"),
        P("seq", "nbr"),
        P("seq", "nbr"),
        P("nbr", "seq"),
    )
    return jax.shard_map(
        body,
        mesh=mesh,
        in_specs=placed,
        out_specs=(
            P(("batch", "seq"), "nbr"),
            P(("batch", "seq"), "nbr"),
            P(("batch", "seq", "nbr"), None, None),
            P(("batch", "nbr"), "seq"),
            P(("batch", "seq"), "nbr"),
            P(("batch", "seq"), "nbr"),
        ),
        check_vma=False,
    )
```
